512 devices in a mesh: blocks: 2 (over y), gz: 128 (over z, x), gy: 2 (over core).
Axes of the slice: x: 8, y: 2, z: 16, core: 2. Of those that a mesh axis runs over, the one named last changes fastest.
The devices are a block of a 8x8x16 slice.
Arguments:
- view_a: float32 [4096, 32, 512], P(('blocks', 'gz'), 'gy'), parts along dimension 0, may hold values from 0.5 to 2
- view_b_own: float32 [1024, 32, 2048], P(('blocks', 'gz'), 'gy'), parts along dimension 0, may hold values from 0.5 to 2
- spread_a: float32 [3, 31], replicated, may hold values from 0.05 to 1
- spread_b: float32 [3, 31], replicated, may hold values from 0.05 to 1
Outputs:
- estimate: float32 [4096, 32, 512], P(('blocks', 'gz'), 'gy'), parts along dimension 0
The draws below stay inside these ranges and needn't reach their ends.
There are 2 independent parts, one for each index of `blocks`. The reference program is written for one: setup_inputs(seed, part) draws one part's arguments, and reference() takes and returns one part's arrays. A program takes and returns all parts, laid end to end along the dimension named above; an argument that names none is the same for every part. Nothing has to cross between parts.
All inputs are finite; a program needn't handle non-finite values.
Results may differ from the reference program's by a relative error of at most 0.0001.
Values sent between devices are 32-bit elements; how exact they have to be, the bound alone decides.
No kernel may reach another device: no remote copies, remote signals or barrier semaphores. Data moves between devices by JAX's collectives and lax.ppermute only.
A program may use at most 64 MiB of HBM per device.

```python
import math
import jax
import jax.numpy as jnp
from jax import lax

NX = 512
R = 15
ITERS = 1
NZ = 2048
NY = 32


def level_of(key, extent, split, smallest, high):
    gain, own = 1.0, jax.random.fold_in(key, 6)
    for position, blocks in split:
        steps = jnp.exp(jax.random.uniform(jax.random.fold_in(own, position), (blocks,), jnp.float32, smallest / len(split), high / len(split)))
        gain = gain * jnp.repeat(steps, extent[position] // blocks).reshape([-1 if axis == position else 1 for axis in range(len(extent))])
    return gain


def setup_inputs(seed: int = 0, part: int = 0) -> dict:
    key_of = jax.random.split(jax.random.key(seed), 5)
    own_keys = jax.random.split(jax.random.fold_in(key_of[4], part), 5)
    return {
        "view_a": jnp.clip(0.5 + 1.5 * jax.random.uniform(own_keys[0], (NZ, NY, NX), jnp.float32) ** level_of(own_keys[0], (NZ, NY, NX), ((0, 128), (1, 2)), -0.2, 0.2), 0.5, 2.0),
        "view_b_own": jnp.clip(0.5 + 1.5 * jax.random.uniform(own_keys[1], (NX, NY, NZ), jnp.float32) ** level_of(own_keys[1], (NX, NY, NZ), ((0, 128), (1, 2)), -0.2, 0.2), 0.5, 2.0),
        "spread_a": jnp.clip(jnp.exp(jax.random.uniform(key_of[2], (3, 2 * R + 1), jnp.float32, math.log(0.05), math.log(1.0))), 0.05, 1.0),
        "spread_b": jnp.clip(jnp.exp(jax.random.uniform(key_of[3], (3, 2 * R + 1), jnp.float32, math.log(0.05), math.log(1.0))), 0.05, 1.0),
    }


def band_table(weights, count_in, count_out, offset):
    source = jnp.arange(count_in, dtype=jnp.int32)[:, None]
    target = jnp.arange(count_out, dtype=jnp.int32)[None, :]
    spread = source - target + offset
    table = jnp.zeros((count_in, count_out), jnp.float32)
    for place in range(weights.shape[0]):
        table = table + jnp.where(spread == place, weights[place], jnp.float32(0.0))
    return table


def blur(volume, kernels):
    padded_x = jnp.pad(volume, ((0, 0), (0, 0), (R, R)))
    along_x = jnp.zeros_like(volume)
    for tap_index in range(2 * R + 1):
        along_x = along_x + kernels[2, tap_index] * padded_x[:, :, tap_index:tap_index + NX]
    table_y = band_table(kernels[1], NY, NY, R)
    along_y = jnp.einsum("zyx,yw->zwx", along_x, table_y, precision=lax.Precision.HIGHEST)
    padded = jnp.pad(along_y, ((R, R), (0, 0), (0, 0)))
    total = jnp.zeros_like(along_y)
    for tap_index in range(2 * R + 1):
        total = total + kernels[0, tap_index] * padded[tap_index:tap_index + NZ]
    return total


def reference(view_a, view_b_own, spread_a, spread_b):
    view_b = jnp.transpose(view_b_own, (2, 1, 0))[:, :, ::-1]
    blur_a = spread_a / jnp.sum(spread_a, axis=1, keepdims=True)
    blur_b = spread_b / jnp.sum(spread_b, axis=1, keepdims=True)
    estimate = 0.5 * (view_a + view_b)
    for iteration in range(ITERS):
        for measured, kernels in ((view_a, blur_a), (view_b, blur_b)):
            quotient = measured / blur(estimate, kernels)
            estimate = estimate * blur(quotient, kernels[:, ::-1])
    return estimate
```

```python
import functools

import jax
import jax.numpy as jnp
from jax import lax
from jax.experimental import pallas as pl
from jax.experimental.pallas import tpu as pltpu
from jax.sharding import PartitionSpec as P

BF16 = jnp.bfloat16
F32 = jnp.float32
MIB = 1 << 20


def halves(values):
    high = values.astype(BF16)
    low = (values - high.astype(F32)).astype(BF16)
    return high, low


def product(left, right):
    dot = functools.partial(jnp.dot, preferred_element_type=F32)
    return dot(left[0], right[0]) + (dot(left[0], right[1]) + dot(left[1], right[0]))


def pick(weights, axis, place, shape):
    spread, flipped = weights
    taps = spread.shape[1]
    table = jnp.zeros(shape, F32)
    total = jnp.zeros(shape[-2:], F32)[:1, :1]
    for tap in range(taps):
        value = spread[axis, taps - 1 - tap if flipped else tap]
        table = jnp.where(place == tap, value, table)
        total = total + value
    return table / total


def put(high_ref, low_ref, where, values):
    high, low = halves(values)
    high_ref[where] = high
    low_ref[where] = low


def tables_kernel(planes, rows, flipped, spread_ref, core, xh, xl, yh, yl, oh, ol, zh, zl, lh, ll, rh, rl):
    weights = (spread_ref, flipped)
    radius = spread_ref.shape[1] // 2
    count_x = xh.shape[0]
    lane = 128
    spread = lax.broadcasted_iota(jnp.int32, (lane, lane), 0) - lax.broadcasted_iota(jnp.int32, (lane, lane), 1)
    blocks = {
        shift: halves(pick(weights, 2, spread + (radius + shift * lane), (lane, lane)))
        for shift in (-1, 0, 1)
    }
    nothing = jnp.zeros((lane, lane), BF16)
    for row in range(count_x // lane):
        for column in range(count_x // lane):
            where = (slice(row * lane, (row + 1) * lane), slice(column * lane, (column + 1) * lane))
            high, low = blocks.get(row - column, (nothing, nothing))
            xh[where] = high
            xl[where] = low
    cells = planes * rows
    edge = radius * rows
    target = lax.broadcasted_iota(jnp.int32, (rows, cells), 0)
    column = lax.broadcasted_iota(jnp.int32, (rows, cells), 1)
    source, plane = column % rows, column // rows
    near = pick(weights, 1, source - target + radius, (rows, cells))
    side = rows * (1 - 2 * core[0])
    far = pick(weights, 1, source - target + radius + side, (rows, cells))
    same = source == target
    edge_same, edge_plane = same[:, :edge], plane[:, :edge]

    def one_plane(at, carry):
        where = (pl.ds(pl.multiple_of(at * rows, rows), rows), slice(None))
        zero = jnp.zeros((), F32)
        put(yh, yl, where, jnp.where(plane == at, near, zero))
        put(oh, ol, where, jnp.where(plane == at, far, zero))
        middle = pick(weights, 0, plane - at + radius, (rows, cells))
        put(zh, zl, where, jnp.where(same, middle, zero))
        left = pick(weights, 0, edge_plane - at, (rows, edge))
        put(lh, ll, where, jnp.where(edge_same, left, zero))
        right = pick(weights, 0, edge_plane - at + (planes + radius), (rows, edge))
        put(rh, rl, where, jnp.where(edge_same, right, zero))
        return carry

    lax.fori_loop(0, planes, one_plane, 0)


def vmem(count):
    return [pl.BlockSpec(memory_space=pltpu.VMEM)] * count


def params(mib):
    return pltpu.CompilerParams(vmem_limit_bytes=mib * MIB)


def cost(flops, moved):
    return pl.CostEstimate(flops=flops, bytes_accessed=moved, transcendentals=0)


def tables(spread, flipped, core, planes, rows, count_x):
    radius = spread.shape[1] // 2
    cells, edge = planes * rows, radius * rows
    shapes = [(count_x, count_x), (cells, cells), (cells, cells), (cells, cells), (cells, edge), (cells, edge)]
    out = [jax.ShapeDtypeStruct(shape, BF16) for shape in shapes for _ in range(2)]
    return pl.pallas_call(
        functools.partial(tables_kernel, planes, rows, flipped),
        out_shape=out,
        in_specs=[pl.BlockSpec(memory_space=pltpu.SMEM)] * 2,
        out_specs=vmem(len(out)),
        compiler_params=params(6),
        cost_estimate=cost(10**7, 4 * 10**6),
        name="tables",
    )(spread, core)


def pack_kernel(planes, own, messages):
    lane = 128
    half = planes // 2
    for block in range(own.shape[1] // lane):
        turned = own[:, block * lane:(block + 1) * lane].T
        for slab in range(lane // planes):
            at = slab * planes
            tile = jnp.concatenate([turned[at:at + half], turned[at + half:at + planes]], axis=1)
            to = block * (lane // planes) + slab
            messages[to * half:(to + 1) * half, :] = tile


def pack(own, planes):
    per_slab, rows, count_z = own.shape
    return pl.pallas_call(
        functools.partial(pack_kernel, planes),
        out_shape=jax.ShapeDtypeStruct((count_z // 2, 2 * per_slab * rows), F32),
        in_specs=vmem(1),
        out_specs=vmem(1)[0],
        compiler_params=params(4),
        cost_estimate=cost(10**6, 10**6),
        name="pack",
    )(own.reshape(per_slab * rows, count_z))


def order_kernel(per_slab, order):
    count_x = order.shape[0]
    slabs = count_x // per_slab
    source = lax.broadcasted_iota(jnp.int32, order.shape, 0)
    target = lax.broadcasted_iota(jnp.int32, order.shape, 1)
    wanted = count_x - 1 - (per_slab * (source % slabs) + source // slabs)
    order[...] = jnp.where(target == wanted, F32(1.0), F32(0.0)).astype(BF16)


def ordering(count_x, per_slab):
    return pl.pallas_call(
        functools.partial(order_kernel, per_slab),
        out_shape=jax.ShapeDtypeStruct((count_x, count_x), BF16),
        out_specs=vmem(1)[0],
        compiler_params=params(4),
        cost_estimate=cost(10**6, 10**6),
        name="ordering",
    )()


def start_kernel(planes, per_slab, messages, view, order, xh, xl, second, estimate, along_x, gathered):
    half = planes // 2
    rows = view.shape[0] // planes
    slabs = messages.shape[0] // half
    for z in range(half):
        turned = messages[pl.ds(z, slabs, stride=half), :].T
        for part in range(2):
            for x in range(per_slab):
                at = (part * per_slab + x) * rows
                to = (part * half + z) * rows
                gathered[to:to + rows, x * slabs:(x + 1) * slabs] = turned[at:at + rows]
    values = gathered[...]
    high = values.astype(BF16)
    rest = values - high.astype(F32)
    middle = rest.astype(BF16)
    low = (rest - middle.astype(F32)).astype(BF16)
    dot = functools.partial(jnp.dot, preferred_element_type=F32)
    moved = (dot(high, order[...]) + dot(middle, order[...])) + dot(low, order[...])
    second[...] = moved
    first = 0.5 * (view[...] + moved)
    estimate[...] = first
    along_x[...] = product(halves(first), (xh[...], xl[...]))


def start(messages, view, order, table, planes):
    cells, count_x = view.shape
    per_slab = count_x * planes // 2 // messages.shape[0]
    block = jax.ShapeDtypeStruct(view.shape, F32)
    return pl.pallas_call(
        functools.partial(start_kernel, planes, per_slab),
        out_shape=[block] * 3,
        in_specs=vmem(5),
        out_specs=vmem(3),
        scratch_shapes=[pltpu.VMEM(view.shape, F32)],
        compiler_params=params(6),
        cost_estimate=cost(10**9, 3 * 10**6),
        name="start",
    )(messages, view, order, *table[0:2])


def across_y_kernel(edge, own, other, yh, yl, oh, ol, whole, head, tail):
    result = product((yh[...], yl[...]), halves(own[...])) + product((oh[...], ol[...]), halves(other[...]))
    whole[...] = result
    head[...] = result[:edge]
    tail[...] = result[result.shape[0] - edge:]


def across_y(own, other, table, edge):
    whole = jax.ShapeDtypeStruct(own.shape, F32)
    piece = jax.ShapeDtypeStruct((edge, own.shape[1]), F32)
    return pl.pallas_call(
        functools.partial(across_y_kernel, edge),
        out_shape=[whole, piece, piece],
        in_specs=vmem(6),
        out_specs=vmem(3),
        compiler_params=params(6),
        cost_estimate=cost(10**9, 3 * 10**6),
        name="across_y",
    )(own, other, *table[2:6])


def across_z_kernel(kind, left, own, right, zh, zl, lh, ll, rh, rl, factor, *rest):
    blurred = product((zh[...], zl[...]), halves(own[...])) + (
        product((lh[...], ll[...]), halves(left[...])) + product((rh[...], rl[...]), halves(right[...]))
    )
    if kind == "last":
        rest[0][...] = factor[...] * blurred
        return
    if kind == "quotient":
        xh, xl, along_x = rest
        value = factor[...] / blurred
    else:
        xh, xl, updated, along_x = rest
        value = factor[...] * blurred
        updated[...] = value
    along_x[...] = product(halves(value), (xh[...], xl[...]))


def across_z(kind, left, own, right, table, factor, following):
    operands = [left, own, right, *table[6:12], factor]
    if kind != "last":
        operands += following[0:2]
    block = jax.ShapeDtypeStruct(own.shape, F32)
    count = 2 if kind == "update" else 1
    return pl.pallas_call(
        functools.partial(across_z_kernel, kind),
        out_shape=[block] * count,
        in_specs=vmem(len(operands)),
        out_specs=vmem(count),
        compiler_params=params(6),
        cost_estimate=cost(10**9, 4 * 10**6),
        name="across_z_" + kind,
    )(*operands)


def shards(view_a, view_b_own, spread_a, spread_b):
    planes, rows, count_x = view_a.shape
    cells = planes * rows
    radius = spread_a.shape[1] // 2
    edge = radius * rows
    slabs = lax.axis_size("gz")
    per_slab = view_b_own.shape[0]
    first = view_a.reshape(cells, count_x)

    packed = pack(view_b_own, planes)
    lanes = packed.shape[1]
    arrived = lax.all_to_all(packed.reshape(slabs, -1, lanes), "gz", 0, 0, tiled=True)
    arrived = arrived.reshape(-1, lanes)

    core = lax.axis_index("gy").astype(jnp.int32).reshape(1)
    steps = [
        tables(spread, flipped, core, planes, rows, count_x)
        for spread in (spread_a, spread_b)
        for flipped in (False, True)
    ]
    order = ordering(count_x, per_slab)

    swap = [(0, 1), (1, 0)]
    up = [(i, i + 1) for i in range(slabs - 1)]
    down = [(i + 1, i) for i in range(slabs - 1)]

    second, estimate, along_x = start(arrived, first, order, steps[0], planes)
    for step, table in enumerate(steps):
        other = lax.ppermute(along_x, "gy", swap)
        whole, head, tail = across_y(along_x, other, table, edge)
        left = lax.ppermute(tail, "gz", up)
        right = lax.ppermute(head, "gz", down)
        if step % 2 == 0:
            measured = first if step == 0 else second
            (along_x,) = across_z("quotient", left, whole, right, table, measured, steps[step + 1])
        elif step + 1 < len(steps):
            estimate, along_x = across_z("update", left, whole, right, table, estimate, steps[step + 1])
        else:
            (estimate,) = across_z("last", left, whole, right, table, estimate, None)
    return estimate.reshape(planes, rows, count_x)


def solution(mesh):
    in_specs = (P(("blocks", "gz"), "gy", None), P(("blocks", "gz"), "gy", None), P(), P())
    out_specs = P(("blocks", "gz"), "gy", None)
    return jax.shard_map(shards, mesh=mesh, in_specs=in_specs, out_specs=out_specs, check_vma=False)
```

```python
import functools

import jax
import jax.numpy as jnp
from jax import lax
from jax.experimental import pallas as pl
from jax.experimental.pallas import tpu as pltpu
from jax.sharding import PartitionSpec as P

BF16 = jnp.bfloat16
F32 = jnp.float32
MIB = 1 << 20


def halves(values):
    high = values.astype(BF16)
    low = (values - high.astype(F32)).astype(BF16)
    return high, low


def product(left, right):
    dot = functools.partial(jnp.dot, preferred_element_type=F32)
    return dot(left[0], right[0]) + (dot(left[0], right[1]) + dot(left[1], right[0]))


def pick(weights, axis, place, shape):
    spread, flipped = weights
    taps = spread.shape[1]
    table = jnp.zeros(shape, F32)
    total = jnp.zeros(shape[-2:], F32)[:1, :1]
    for tap in range(taps):
        value = spread[axis, taps - 1 - tap if flipped else tap]
        table = jnp.where(place == tap, value, table)
        total = total + value
    return table / total


def put(high_ref, low_ref, where, values):
    high, low = halves(values)
    high_ref[where] = high
    low_ref[where] = low


def tables_kernel(planes, rows, flipped, spread_ref, core, xh, xl, yh, yl, oh, ol, zh, zl, lh, ll, rh, rl):
    weights = (spread_ref, flipped)
    radius = spread_ref.shape[1] // 2
    count_x = xh.shape[0]
    lane = 128
    spread = lax.broadcasted_iota(jnp.int32, (lane, lane), 0) - lax.broadcasted_iota(jnp.int32, (lane, lane), 1)
    blocks = {
        shift: halves(pick(weights, 2, spread + (radius + shift * lane), (lane, lane)))
        for shift in (-1, 0, 1)
    }
    nothing = jnp.zeros((lane, lane), BF16)
    for row in range(count_x // lane):
        for column in range(count_x // lane):
            where = (slice(row * lane, (row + 1) * lane), slice(column * lane, (column + 1) * lane))
            high, low = blocks.get(row - column, (nothing, nothing))
            xh[where] = high
            xl[where] = low
    cells = planes * rows
    edge = radius * rows
    target = lax.broadcasted_iota(jnp.int32, (rows, cells), 0)
    column = lax.broadcasted_iota(jnp.int32, (rows, cells), 1)
    source, plane = column % rows, column // rows
    near = pick(weights, 1, source - target + radius, (rows, cells))
    side = rows * (1 - 2 * core[0])
    far = pick(weights, 1, source - target + radius + side, (rows, cells))
    same = source == target
    edge_same, edge_plane = same[:, :edge], plane[:, :edge]
    beyond = planes + radius

    def one_plane(at, carry):
        where = (pl.ds(pl.multiple_of(at * rows, rows), rows), slice(None))
        zero = jnp.zeros((), F32)
        put(yh, yl, where, jnp.where(plane == at, near, zero))
        put(oh, ol, where, jnp.where(plane == at, far, zero))
        middle = pick(weights, 0, plane - at + radius, (rows, cells))
        put(zh, zl, where, jnp.where(same, middle, zero))
        below = pick(weights, 0, edge_plane - at + core[0] * beyond, (rows, edge))
        put(lh, ll, where, jnp.where(edge_same, below, zero))
        above = pick(weights, 0, edge_plane - at + (1 - core[0]) * beyond, (rows, edge))
        put(rh, rl, where, jnp.where(edge_same, above, zero))
        return carry

    lax.fori_loop(0, planes, one_plane, 0)


def vmem(count):
    return [pl.BlockSpec(memory_space=pltpu.VMEM)] * count


def params(mib):
    return pltpu.CompilerParams(vmem_limit_bytes=mib * MIB)


def cost(flops, moved):
    return pl.CostEstimate(flops=flops, bytes_accessed=moved, transcendentals=0)


def tables(spread, flipped, core, planes, rows, count_x):
    radius = spread.shape[1] // 2
    cells, edge = planes * rows, radius * rows
    shapes = [(count_x, count_x), (cells, cells), (cells, cells), (cells, cells), (cells, edge), (cells, edge)]
    out = [jax.ShapeDtypeStruct(shape, BF16) for shape in shapes for _ in range(2)]
    return pl.pallas_call(
        functools.partial(tables_kernel, planes, rows, flipped),
        out_shape=out,
        in_specs=[pl.BlockSpec(memory_space=pltpu.SMEM)] * 2,
        out_specs=vmem(len(out)),
        compiler_params=params(6),
        cost_estimate=cost(10**7, 4 * 10**6),
        name="tables",
    )(spread, core)


def pack_kernel(planes, own, messages):
    lane = 128
    half = planes // 2
    for block in range(own.shape[1] // lane):
        turned = own[:, block * lane:(block + 1) * lane].T
        for slab in range(lane // planes):
            at = slab * planes
            tile = jnp.concatenate([turned[at:at + half], turned[at + half:at + planes]], axis=1)
            to = block * (lane // planes) + slab
            messages[to * half:(to + 1) * half, :] = tile


def pack(own, planes):
    per_slab, rows, count_z = own.shape
    return pl.pallas_call(
        functools.partial(pack_kernel, planes),
        out_shape=jax.ShapeDtypeStruct((count_z // 2, 2 * per_slab * rows), F32),
        in_specs=vmem(1),
        out_specs=vmem(1)[0],
        compiler_params=params(4),
        cost_estimate=cost(10**6, 10**6),
        name="pack",
    )(own.reshape(per_slab * rows, count_z))


def order_kernel(per_slab, order):
    count_x = order.shape[0]
    slabs = count_x // per_slab
    source = lax.broadcasted_iota(jnp.int32, order.shape, 0)
    target = lax.broadcasted_iota(jnp.int32, order.shape, 1)
    wanted = count_x - 1 - (per_slab * (source % slabs) + source // slabs)
    order[...] = jnp.where(target == wanted, F32(1.0), F32(0.0)).astype(BF16)


def ordering(count_x, per_slab):
    return pl.pallas_call(
        functools.partial(order_kernel, per_slab),
        out_shape=jax.ShapeDtypeStruct((count_x, count_x), BF16),
        out_specs=vmem(1)[0],
        compiler_params=params(4),
        cost_estimate=cost(10**6, 10**6),
        name="ordering",
    )()


def start_kernel(planes, per_slab, messages, view, order, xh, xl, second, estimate, along_x, gathered):
    half = planes // 2
    rows = view.shape[0] // planes
    slabs = messages.shape[0] // half
    for z in range(half):
        turned = messages[pl.ds(z, slabs, stride=half), :].T
        for part in range(2):
            for x in range(per_slab):
                at = (part * per_slab + x) * rows
                to = (part * half + z) * rows
                gathered[to:to + rows, x * slabs:(x + 1) * slabs] = turned[at:at + rows]
    values = gathered[...]
    high = values.astype(BF16)
    rest = values - high.astype(F32)
    middle = rest.astype(BF16)
    low = (rest - middle.astype(F32)).astype(BF16)
    dot = functools.partial(jnp.dot, preferred_element_type=F32)
    moved = (dot(high, order[...]) + dot(middle, order[...])) + dot(low, order[...])
    second[...] = moved
    first = 0.5 * (view[...] + moved)
    estimate[...] = first
    along_x[...] = product(halves(first), (xh[...], xl[...]))


def start(messages, view, order, table, planes):
    cells, count_x = view.shape
    per_slab = count_x * planes // 2 // messages.shape[0]
    block = jax.ShapeDtypeStruct(view.shape, F32)
    return pl.pallas_call(
        functools.partial(start_kernel, planes, per_slab),
        out_shape=[block] * 3,
        in_specs=vmem(5),
        out_specs=vmem(3),
        scratch_shapes=[pltpu.VMEM(view.shape, F32)],
        compiler_params=params(6),
        cost_estimate=cost(10**9, 3 * 10**6),
        name="start",
    )(messages, view, order, *table[0:2])


def across_y_kernel(edge, core, own, other, yh, yl, oh, ol, whole, first, second):
    whole[...] = product((yh[...], yl[...]), halves(own[...])) + product((oh[...], ol[...]), halves(other[...]))
    inner = whole.shape[0] - edge
    first[...] = whole[pl.ds(pl.multiple_of((1 - core[0]) * inner, inner), edge), :]
    second[...] = whole[pl.ds(pl.multiple_of(core[0] * inner, inner), edge), :]


def across_y(core, own, other, table, edge):
    whole = jax.ShapeDtypeStruct(own.shape, F32)
    piece = jax.ShapeDtypeStruct((edge, own.shape[1]), F32)
    return pl.pallas_call(
        functools.partial(across_y_kernel, edge),
        out_shape=[whole, piece, piece],
        in_specs=[pl.BlockSpec(memory_space=pltpu.SMEM)] + vmem(6),
        out_specs=vmem(3),
        compiler_params=params(6),
        cost_estimate=cost(10**9, 3 * 10**6),
        name="across_y",
    )(core, own, other, *table[2:6])


def across_z_kernel(kind, left, own, right, zh, zl, lh, ll, rh, rl, factor, *rest):
    blurred = product((zh[...], zl[...]), halves(own[...])) + (
        product((lh[...], ll[...]), halves(left[...])) + product((rh[...], rl[...]), halves(right[...]))
    )
    if kind == "last":
        rest[0][...] = factor[...] * blurred
        return
    if kind == "quotient":
        xh, xl, along_x = rest
        value = factor[...] / blurred
    else:
        xh, xl, updated, along_x = rest
        value = factor[...] * blurred
        updated[...] = value
    along_x[...] = product(halves(value), (xh[...], xl[...]))


def across_z(kind, left, own, right, table, factor, following):
    operands = [left, own, right, *table[6:12], factor]
    if kind != "last":
        operands += following[0:2]
    block = jax.ShapeDtypeStruct(own.shape, F32)
    count = 2 if kind == "update" else 1
    return pl.pallas_call(
        functools.partial(across_z_kernel, kind),
        out_shape=[block] * count,
        in_specs=vmem(len(operands)),
        out_specs=vmem(count),
        compiler_params=params(6),
        cost_estimate=cost(10**9, 4 * 10**6),
        name="across_z_" + kind,
    )(*operands)


def shards(view_a, view_b_own, spread_a, spread_b):
    planes, rows, count_x = view_a.shape
    cells = planes * rows
    radius = spread_a.shape[1] // 2
    edge = radius * rows
    slabs = lax.axis_size("gz")
    per_slab = view_b_own.shape[0]
    first = view_a.reshape(cells, count_x)

    packed = pack(view_b_own, planes)
    lanes = packed.shape[1]
    arrived = lax.all_to_all(packed.reshape(slabs, -1, lanes), "gz", 0, 0, tiled=True)
    arrived = arrived.reshape(-1, lanes)

    core = lax.axis_index("gy").astype(jnp.int32).reshape(1)
    steps = [
        tables(spread, flipped, core, planes, rows, count_x)
        for spread in (spread_a, spread_b)
        for flipped in (False, True)
    ]
    order = ordering(count_x, per_slab)

    swap = [(0, 1), (1, 0)]
    up = [[(2 * i + core, 2 * i + 2 + core) for i in range(slabs - 1)] for core in range(2)]
    down = [[(2 * i + 2 + core, 2 * i + core) for i in range(slabs - 1)] for core in range(2)]

    second, estimate, along_x = start(arrived, first, order, steps[0], planes)
    for step, table in enumerate(steps):
        other = lax.ppermute(along_x, "gy", swap)
        whole, before, after = across_y(core, along_x, other, table, edge)
        left = lax.ppermute(before, ("gz", "gy"), up[0] + down[1])
        right = lax.ppermute(after, ("gz", "gy"), down[0] + up[1])
        if step % 2 == 0:
            measured = first if step == 0 else second
            (along_x,) = across_z("quotient", left, whole, right, table, measured, steps[step + 1])
        elif step + 1 < len(steps):
            estimate, along_x = across_z("update", left, whole, right, table, estimate, steps[step + 1])
        else:
            (estimate,) = across_z("last", left, whole, right, table, estimate, None)
    return estimate.reshape(planes, rows, count_x)


def solution(mesh):
    in_specs = (P(("blocks", "gz"), "gy", None), P(("blocks", "gz"), "gy", None), P(), P())
    out_specs = P(("blocks", "gz"), "gy", None)
    return jax.shard_map(shards, mesh=mesh, in_specs=in_specs, out_specs=out_specs, check_vma=False)
```

```python
import functools

import jax
import jax.numpy as jnp
from jax import lax
from jax.experimental import pallas as pl
from jax.experimental.pallas import tpu as pltpu
from jax.sharding import PartitionSpec as P


BF16 = jnp.bfloat16
F32 = jnp.float32
MIB = 1 << 20


def halves(values):
    high = values.astype(BF16)
    low = (values - high.astype(F32)).astype(BF16)
    return high, low


def product(left, right):
    dot = functools.partial(jnp.dot, preferred_element_type=F32)
    return dot(left[0], right[0]) + (dot(left[0], right[1]) + dot(left[1], right[0]))


def pick(weights, axis, place):
    spread, flipped = weights
    taps = spread.shape[1]
    table = jnp.zeros(place.shape, F32)
    total = jnp.zeros((1, 1), F32)
    for tap in range(taps):
        value = spread[axis, taps - 1 - tap if flipped else tap]
        table = jnp.where(place == tap, value, table)
        total = total + value
    return table / total


def put(high_ref, low_ref, where, values):
    high, low = halves(values)
    high_ref[where] = high
    low_ref[where] = low


SHIFTS = ((0, 0), (1, -1), (2, -2), (-1, 1), (None, 2))


def tables_kernel(planes, rows, flipped, spread_ref, core, xh, xl, yh, yl, *zs):
    weights = (spread_ref, flipped)
    radius = spread_ref.shape[1] // 2
    count_x = xh.shape[0]
    lane = 128
    spread = lax.broadcasted_iota(jnp.int32, (lane, lane), 0) - lax.broadcasted_iota(jnp.int32, (lane, lane), 1)
    blocks = {shift: halves(pick(weights, 2, spread + (radius + shift * lane))) for shift in (-1, 0, 1)}
    nothing = jnp.zeros((lane, lane), BF16)
    for row in range(count_x // lane):
        for column in range(count_x // lane):
            where = (slice(row * lane, (row + 1) * lane), slice(column * lane, (column + 1) * lane))
            high, low = blocks.get(row - column, (nothing, nothing))
            xh[where] = high
            xl[where] = low
    half = planes // 2
    count = half * rows
    zero = jnp.zeros((), F32)

    def places(length, shape):
        column = lax.broadcasted_iota(jnp.int32, shape, 1)
        return column // length, (column % length) // rows, column % rows

    target = lax.broadcasted_iota(jnp.int32, (rows, 2 * count), 0)
    part, plane, cell = places(count, (rows, 2 * count))
    across = [pick(weights, 1, rows * (part - side) + cell - target + radius) for side in range(2)]
    pieces = []
    for position, (south, north) in enumerate(SHIFTS):
        length = zs[2 * position].shape[1] // 2
        base = radius * -1 if south is None else south * half
        shift = jnp.where(core[0] == 0, base, north * half)
        side_of, _, cell_of = places(length, (rows, 2 * length))
        same = cell_of == lax.broadcasted_iota(jnp.int32, (rows, 2 * length), 0)
        near = places(length, (8, 2 * length))[1] + (shift + radius)
        pieces.append((zs[2 * position], zs[2 * position + 1], near, side_of, same))

    def one_plane(at, carry):
        values = [pick(weights, 0, near - at) for _, _, near, _, _ in pieces]
        for side in range(2):
            where = (pl.ds(pl.multiple_of(side * count + at * rows, rows), rows), slice(None))
            put(yh, yl, where, jnp.where(plane == at, across[side], zero))
            for (high, low, _, side_of, same), value in zip(pieces, values):
                spread_out = jnp.concatenate([value] * (rows // 8), axis=0)
                put(high, low, where, jnp.where(same & (side_of == side), spread_out, zero))
        return carry

    lax.fori_loop(0, half, one_plane, 0)


def vmem(count):
    return [pl.BlockSpec(memory_space=pltpu.VMEM)] * count


def smem(count):
    return [pl.BlockSpec(memory_space=pltpu.SMEM)] * count


def params(mib):
    return pltpu.CompilerParams(vmem_limit_bytes=mib * MIB)


def cost(flops, moved):
    return pl.CostEstimate(flops=flops, bytes_accessed=moved, transcendentals=0)


def tables(spread, flipped, core, planes, rows, count_x):
    cells = planes * rows
    short = 2 * (spread.shape[1] // 2 - planes // 2) * rows
    shapes = [(count_x, count_x)] + [(cells, cells)] * 5 + [(cells, short)]
    out = [jax.ShapeDtypeStruct(shape, BF16) for shape in shapes for _ in range(2)]
    return pl.pallas_call(
        functools.partial(tables_kernel, planes, rows, flipped),
        out_shape=out,
        in_specs=smem(2),
        out_specs=vmem(len(out)),
        compiler_params=params(6),
        cost_estimate=cost(10**7, 4 * 10**6),
        name="tables",
    )(spread, core)


def pack_kernel(planes, own, messages):
    lane = 128
    half = planes // 2
    for block in range(own.shape[1] // lane):
        turned = own[:, block * lane:(block + 1) * lane].T
        for slab in range(lane // planes):
            at = slab * planes
            tile = jnp.concatenate([turned[at:at + half], turned[at + half:at + planes]], axis=1)
            to = block * (lane // planes) + slab
            messages[to * half:(to + 1) * half, :] = tile


def pack(own, planes):
    per_slab, rows, count_z = own.shape
    return pl.pallas_call(
        functools.partial(pack_kernel, planes),
        out_shape=jax.ShapeDtypeStruct((count_z // 2, 2 * per_slab * rows), F32),
        in_specs=vmem(1),
        out_specs=vmem(1)[0],
        compiler_params=params(4),
        cost_estimate=cost(10**6, 10**6),
        name="pack",
    )(own.reshape(per_slab * rows, count_z))


def order_kernel(per_slab, order):
    count_x = order.shape[0]
    slabs = count_x // per_slab
    source = lax.broadcasted_iota(jnp.int32, order.shape, 0)
    target = lax.broadcasted_iota(jnp.int32, order.shape, 1)
    wanted = count_x - 1 - (per_slab * (source % slabs) + source // slabs)
    order[...] = jnp.where(target == wanted, F32(1.0), F32(0.0)).astype(BF16)


def ordering(count_x, per_slab):
    return pl.pallas_call(
        functools.partial(order_kernel, per_slab),
        out_shape=jax.ShapeDtypeStruct((count_x, count_x), BF16),
        out_specs=vmem(1)[0],
        compiler_params=params(4),
        cost_estimate=cost(10**6, 10**6),
        name="ordering",
    )()


def parted(core, values_ref, keep, give):
    count = keep.shape[0]
    keep[...] = values_ref[pl.ds(pl.multiple_of(core[0] * count, count), count), :]
    give[...] = values_ref[pl.ds(pl.multiple_of((1 - core[0]) * count, count), count), :]


def joined(core, keep, got, values_ref):
    count = keep.shape[0]
    values_ref[pl.ds(pl.multiple_of(core[0] * count, count), count), :] = keep[...]
    values_ref[pl.ds(pl.multiple_of((1 - core[0]) * count, count), count), :] = got[...]


def call(kernel, scalars, operands, shapes, scratch=()):
    return pl.pallas_call(
        kernel,
        out_shape=[jax.ShapeDtypeStruct(shape, F32) for shape in shapes],
        in_specs=smem(len(scalars)) + vmem(len(operands)),
        out_specs=vmem(len(shapes)),
        scratch_shapes=[pltpu.VMEM(shape, F32) for shape in scratch],
        compiler_params=params(6),
        cost_estimate=cost(10**9, 3 * 10**6),
    )(*scalars, *operands)


def start_kernel(planes, per_slab, core, messages, view, order, xh, xl, kept, given, kept_x, given_x, gathered, whole):
    half = planes // 2
    rows = view.shape[0] // planes
    slabs = messages.shape[0] // half
    for z in range(half):
        turned = messages[pl.ds(z, slabs, stride=half), :].T
        for part in range(2):
            for x in range(per_slab):
                at = (part * per_slab + x) * rows
                to = (part * half + z) * rows
                gathered[to:to + rows, x * slabs:(x + 1) * slabs] = turned[at:at + rows]
    values = gathered[...]
    high = values.astype(BF16)
    rest = values - high.astype(F32)
    middle = rest.astype(BF16)
    low = (rest - middle.astype(F32)).astype(BF16)
    dot = functools.partial(jnp.dot, preferred_element_type=F32)
    moved = (dot(high, order[...]) + dot(middle, order[...])) + dot(low, order[...])
    whole[...] = moved
    parted(core, whole, kept, given)
    whole[...] = product(halves(0.5 * (view[...] + moved)), (xh[...], xl[...]))
    parted(core, whole, kept_x, given_x)


def part_kernel(core, values, keep, give):
    parted(core, values, keep, give)


def join_kernel(core, keep, got, values):
    joined(core, keep, got, values)


def join_both_kernel(core, keep, got, view, values, estimate):
    joined(core, keep, got, values)
    estimate[...] = 0.5 * (view[...] + values[...])


def send_y(core, values, yh, yl, whole, second):
    whole[...] = product((yh[...], yl[...]), halves(values))
    count = whole.shape[0] // 2
    length = second.shape[0] // 2
    skipped = (1 - core[0]) * (count - length)
    for side in range(2):
        at = pl.multiple_of(side * count + skipped, count - length)
        second[side * length:(side + 1) * length, :] = whole[pl.ds(at, length), :]


def enter_kernel(core, keep, got, yh, yl, whole, second, values):
    joined(core, keep, got, values)
    send_y(core, values[...], yh, yl, whole, second)


def partial_kernel(pieces, *refs):
    total = None
    for piece in range(pieces):
        high, low, values = refs[3 * piece:3 * piece + 3]
        term = product((high[...], low[...]), halves(values[...]))
        total = term if total is None else total + term
    for more in refs[3 * pieces:-1]:
        total = total + more[...]
    refs[-1][...] = total


def partial(terms, more=()):
    operands = [operand for high, low, values in terms for operand in (high, low, values)]
    return call(functools.partial(partial_kernel, len(terms)), (), [*operands, *more], [terms[0][2].shape])[0]


def finish_kernel(kind, core, part, second, sh, sl, factor, *rest):
    blurred = part[...] + product((sh[...], sl[...]), halves(second[...]))
    if kind == "last":
        keep, give, values = rest
        values[...] = factor[...] * blurred
        parted(core, values, keep, give)
        return
    xh, xl, yh, yl, *outs = rest
    if kind == "quotient":
        value = factor[...] / blurred
    else:
        value = factor[...] * blurred
        outs[0][...] = value
    along_x = product(halves(value), (xh[...], xl[...]))
    send_y(core, along_x, yh, yl, outs[-2], outs[-1])


def finish(kind, core, part, second, table, factor, following):
    operands = [part, second, *table[12:14], factor]
    block = part.shape
    if kind == "last":
        piece = (block[0] // 2, block[1])
        shapes, scratch = [piece, piece], [block]
    else:
        operands += following[0:4]
        shapes, scratch = [block, second.shape], []
        if kind == "update":
            shapes = [block] + shapes
    return call(functools.partial(finish_kernel, kind), [core], operands, shapes, scratch)


def shards(view_a, view_b_own, spread_a, spread_b):
    planes, rows, count_x = view_a.shape
    cells = planes * rows
    short = 2 * (spread_a.shape[1] // 2 - planes // 2) * rows
    slabs = lax.axis_size("gz")
    per_slab = view_b_own.shape[0]
    first_y = view_a.reshape(cells, count_x)
    block, piece, ends = (cells, count_x), (cells // 2, count_x), (short, count_x)

    core = lax.axis_index("gy").astype(jnp.int32).reshape(1)
    swap = [(0, 1), (1, 0)]
    up = [[(2 * i + core, 2 * i + 2 + core) for i in range(slabs - 1)] for core in range(2)]
    down = [[(2 * i + 2 + core, 2 * i + core) for i in range(slabs - 1)] for core in range(2)]

    def table_of(step):
        return tables((spread_a, spread_b)[step // 2], step % 2 == 1, core, planes, rows, count_x)

    packed = pack(view_b_own, planes)
    lanes = packed.shape[1]
    arrived = lax.all_to_all(packed.reshape(slabs, -1, lanes), "gz", 0, 0, tiled=True)
    arrived = arrived.reshape(-1, lanes)
    keep, give = call(part_kernel, [core], [first_y], [piece, piece])
    got = lax.ppermute(give, "gy", swap)
    (first,) = call(join_kernel, [core], [keep, got], [block])
    table = table_of(0)
    order = ordering(count_x, per_slab)

    kept, given, kept_x, given_x = call(
        functools.partial(start_kernel, planes, per_slab), [core],
        [arrived, first_y, order, *table[0:2]], [piece] * 4, [block, block],
    )
    got_x = lax.ppermute(given_x, "gy", swap)
    whole, ends_of = call(enter_kernel, [core], [kept_x, got_x, *table[2:4]], [block, ends], [block])

    for step in range(4):
        first_planes = lax.ppermute(whole, ("gz", "gy"), up[1] + down[0])
        side_planes = lax.ppermute(whole, "gy", swap)
        second_planes = lax.ppermute(ends_of, ("gz", "gy"), up[0] + down[1])
        if step < 3:
            following = table_of(step + 1)
        part = partial([(*table[4:6], whole), (*table[6:8], side_planes)])
        forward_planes = lax.ppermute(first_planes, "gy", swap)
        part = partial([(*table[8:10], first_planes)], [part])
        if step == 0:
            got_b = lax.ppermute(given, "gy", swap)
            second, estimate = call(join_both_kernel, [core], [kept, got_b, first], [block, block])
        part = partial([(*table[10:12], forward_planes)], [part])
        arrivals = (core, part, second_planes, table)
        if step % 2 == 0:
            measured = first if step == 0 else second
            whole, ends_of = finish("quotient", *arrivals, measured, following)
        elif step < 3:
            estimate, whole, ends_of = finish("update", *arrivals, estimate, following)
        else:
            keep, give = finish("last", *arrivals, estimate, None)
        table = following
    got = lax.ppermute(give, "gy", swap)
    (estimate,) = call(join_kernel, [core], [keep, got], [block])
    return estimate.reshape(planes, rows, count_x)


def solution(mesh):
    in_specs = (P(("blocks", "gz"), "gy", None), P(("blocks", "gz"), "gy", None), P(), P())
    out_specs = P(("blocks", "gz"), "gy", None)
    return jax.shard_map(shards, mesh=mesh, in_specs=in_specs, out_specs=out_specs, check_vma=False)
```

```python
import functools

import jax
import jax.numpy as jnp
from jax import lax
from jax.experimental import pallas as pl
from jax.experimental.pallas import tpu as pltpu
from jax.sharding import PartitionSpec as P


BF16 = jnp.bfloat16
F32 = jnp.float32
MIB = 1 << 20


def halves(values):
    high = values.astype(BF16)
    low = (values - high.astype(F32)).astype(BF16)
    return high, low


def product(left, right):
    dot = functools.partial(jnp.dot, preferred_element_type=F32)
    return dot(left[0], right[0]) + (dot(left[0], right[1]) + dot(left[1], right[0]))


def pick(weights, axis, place):
    spread, flipped = weights
    taps = spread.shape[1]
    table = jnp.zeros(place.shape, F32)
    total = jnp.zeros((1, 1), F32)
    for tap in range(taps):
        value = spread[axis, taps - 1 - tap if flipped else tap]
        table = jnp.where(place == tap, value, table)
        total = total + value
    return table / total


def put(high_ref, low_ref, where, values):
    high, low = halves(values)
    high_ref[where] = high
    low_ref[where] = low


SHIFTS = ((0, 0), (1, -1), (2, -2), (-1, 1), (None, 2))


def tables_kernel(planes, rows, flipped, spread_ref, core, xh, xl, yh, yl, *zs):
    weights = (spread_ref, flipped)
    radius = spread_ref.shape[1] // 2
    count_x = xh.shape[0]
    lane = 128
    spread = lax.broadcasted_iota(jnp.int32, (lane, lane), 0) - lax.broadcasted_iota(jnp.int32, (lane, lane), 1)
    blocks = {shift: halves(pick(weights, 2, spread + (radius + shift * lane))) for shift in (-1, 0, 1)}
    nothing = jnp.zeros((lane, lane), BF16)
    for row in range(count_x // lane):
        for column in range(count_x // lane):
            where = (slice(row * lane, (row + 1) * lane), slice(column * lane, (column + 1) * lane))
            high, low = blocks.get(row - column, (nothing, nothing))
            xh[where] = high
            xl[where] = low
    half = planes // 2
    count = half * rows
    zero = jnp.zeros((), F32)

    def places(length, shape):
        column = lax.broadcasted_iota(jnp.int32, shape, 1)
        return column // length, (column % length) // rows, column % rows

    target = lax.broadcasted_iota(jnp.int32, (rows, 2 * count), 0)
    part, plane, cell = places(count, (rows, 2 * count))
    across = [pick(weights, 1, rows * (part - side) + cell - target + radius) for side in range(2)]
    pieces = []
    for position, (south, north) in enumerate(SHIFTS):
        length = zs[2 * position].shape[1] // 2
        base = radius * -1 if south is None else south * half
        shift = jnp.where(core[0] == 0, base, north * half)
        side_of, _, cell_of = places(length, (rows, 2 * length))
        same = cell_of == lax.broadcasted_iota(jnp.int32, (rows, 2 * length), 0)
        near = places(length, (8, 2 * length))[1] + (shift + radius)
        pieces.append((zs[2 * position], zs[2 * position + 1], near, side_of, same))

    def one_plane(at, carry):
        values = [pick(weights, 0, near - at) for _, _, near, _, _ in pieces]
        for side in range(2):
            where = (pl.ds(pl.multiple_of(side * count + at * rows, rows), rows), slice(None))
            put(yh, yl, where, jnp.where(plane == at, across[side], zero))
            for (high, low, _, side_of, same), value in zip(pieces, values):
                spread_out = jnp.concatenate([value] * (rows // 8), axis=0)
                put(high, low, where, jnp.where(same & (side_of == side), spread_out, zero))
        return carry

    lax.fori_loop(0, half, one_plane, 0)


def vmem(count):
    return [pl.BlockSpec(memory_space=pltpu.VMEM)] * count


def smem(count):
    return [pl.BlockSpec(memory_space=pltpu.SMEM)] * count


def params(mib):
    return pltpu.CompilerParams(vmem_limit_bytes=mib * MIB)


def cost(flops, moved):
    return pl.CostEstimate(flops=flops, bytes_accessed=moved, transcendentals=0)


def tables(spread, flipped, core, planes, rows, count_x):
    cells = planes * rows
    short = 2 * (spread.shape[1] // 2 - planes // 2) * rows
    shapes = [(count_x, count_x)] + [(cells, cells)] * 5 + [(cells, short)]
    out = [jax.ShapeDtypeStruct(shape, BF16) for shape in shapes for _ in range(2)]
    return pl.pallas_call(
        functools.partial(tables_kernel, planes, rows, flipped),
        out_shape=out,
        in_specs=smem(2),
        out_specs=vmem(len(out)),
        compiler_params=params(6),
        cost_estimate=cost(10**7, 4 * 10**6),
        name="tables",
    )(spread, core)


def pack_kernel(planes, own, messages):
    lane = 128
    half = planes // 2
    for block in range(own.shape[1] // lane):
        turned = own[:, block * lane:(block + 1) * lane].T
        for slab in range(lane // planes):
            at = slab * planes
            tile = jnp.concatenate([turned[at:at + half], turned[at + half:at + planes]], axis=1)
            to = block * (lane // planes) + slab
            messages[to * half:(to + 1) * half, :] = tile


def pack(own, planes):
    per_slab, rows, count_z = own.shape
    return pl.pallas_call(
        functools.partial(pack_kernel, planes),
        out_shape=jax.ShapeDtypeStruct((count_z // 2, 2 * per_slab * rows), F32),
        in_specs=vmem(1),
        out_specs=vmem(1)[0],
        compiler_params=params(4),
        cost_estimate=cost(10**6, 10**6),
        name="pack",
    )(own.reshape(per_slab * rows, count_z))


def order_kernel(per_slab, order):
    count_x = order.shape[0]
    slabs = count_x // per_slab
    source = lax.broadcasted_iota(jnp.int32, order.shape, 0)
    target = lax.broadcasted_iota(jnp.int32, order.shape, 1)
    wanted = count_x - 1 - (per_slab * (source % slabs) + source // slabs)
    order[...] = jnp.where(target == wanted, F32(1.0), F32(0.0)).astype(BF16)


def ordering(count_x, per_slab):
    return pl.pallas_call(
        functools.partial(order_kernel, per_slab),
        out_shape=jax.ShapeDtypeStruct((count_x, count_x), BF16),
        out_specs=vmem(1)[0],
        compiler_params=params(4),
        cost_estimate=cost(10**6, 10**6),
        name="ordering",
    )()


def parted(core, values_ref, keep, give):
    count = keep.shape[0]
    keep[...] = values_ref[pl.ds(pl.multiple_of(core[0] * count, count), count), :]
    give[...] = values_ref[pl.ds(pl.multiple_of((1 - core[0]) * count, count), count), :]


def joined(core, keep, got, values_ref):
    count = keep.shape[0]
    values_ref[pl.ds(pl.multiple_of(core[0] * count, count), count), :] = keep[...]
    values_ref[pl.ds(pl.multiple_of((1 - core[0]) * count, count), count), :] = got[...]


def call(kernel, scalars, operands, shapes, scratch=()):
    return pl.pallas_call(
        kernel,
        out_shape=[jax.ShapeDtypeStruct(shape, F32) for shape in shapes],
        in_specs=smem(len(scalars)) + vmem(len(operands)),
        out_specs=vmem(len(shapes)),
        scratch_shapes=[pltpu.VMEM(shape, F32) for shape in scratch],
        compiler_params=params(6),
        cost_estimate=cost(10**9, 3 * 10**6),
    )(*scalars, *operands)


def start_kernel(planes, per_slab, core, messages, view, order, xh, xl, kept, kept_x, given, gathered, whole):
    half = planes // 2
    rows = view.shape[0] // planes
    slabs = messages.shape[0] // half
    for z in range(half):
        turned = messages[pl.ds(z, slabs, stride=half), :].T
        for part in range(2):
            for x in range(per_slab):
                at = (part * per_slab + x) * rows
                to = (part * half + z) * rows
                gathered[to:to + rows, x * slabs:(x + 1) * slabs] = turned[at:at + rows]
    values = gathered[...]
    high = values.astype(BF16)
    rest = values - high.astype(F32)
    middle = rest.astype(BF16)
    low = (rest - middle.astype(F32)).astype(BF16)
    dot = functools.partial(jnp.dot, preferred_element_type=F32)
    moved = (dot(high, order[...]) + dot(middle, order[...])) + dot(low, order[...])
    count = kept.shape[0]
    whole[...] = moved
    parted(core, whole, kept, given.at[count:])
    whole[...] = product(halves(0.5 * (view[...] + moved)), (xh[...], xl[...]))
    parted(core, whole, kept_x, given.at[:count])


def part_kernel(core, values, keep, give):
    parted(core, values, keep, give)


def join_kernel(core, keep, got, values):
    joined(core, keep, got, values)


def join_both_kernel(core, keep, got, view, values, estimate):
    joined(core, keep, got.at[keep.shape[0]:], values)
    estimate[...] = 0.5 * (view[...] + values[...])


def send_y(core, values, yh, yl, whole, second):
    whole[...] = product((yh[...], yl[...]), halves(values))
    count = whole.shape[0] // 2
    length = second.shape[0] // 2
    skipped = (1 - core[0]) * (count - length)
    for side in range(2):
        at = pl.multiple_of(side * count + skipped, count - length)
        second[side * length:(side + 1) * length, :] = whole[pl.ds(at, length), :]


def enter_kernel(core, keep, got, yh, yl, whole, second, values):
    joined(core, keep, got.at[:keep.shape[0]], values)
    send_y(core, values[...], yh, yl, whole, second)


def partial_kernel(pieces, *refs):
    total = None
    for piece in range(pieces):
        high, low, values = refs[3 * piece:3 * piece + 3]
        term = product((high[...], low[...]), halves(values[...]))
        total = term if total is None else total + term
    for more in refs[3 * pieces:-1]:
        total = total + more[...]
    refs[-1][...] = total


def partial(terms, more=()):
    operands = [operand for high, low, values in terms for operand in (high, low, values)]
    return call(functools.partial(partial_kernel, len(terms)), (), [*operands, *more], [terms[0][2].shape])[0]


def finish_kernel(kind, core, part, second, sh, sl, factor, *rest):
    blurred = part[...] + product((sh[...], sl[...]), halves(second[...]))
    if kind == "last":
        keep, give, values = rest
        values[...] = factor[...] * blurred
        parted(core, values, keep, give)
        return
    xh, xl, yh, yl, *outs = rest
    if kind == "quotient":
        value = factor[...] / blurred
    else:
        value = factor[...] * blurred
        outs[0][...] = value
    along_x = product(halves(value), (xh[...], xl[...]))
    send_y(core, along_x, yh, yl, outs[-2], outs[-1])


def finish(kind, core, part, second, table, factor, following):
    operands = [part, second, *table[12:14], factor]
    block = part.shape
    if kind == "last":
        piece = (block[0] // 2, block[1])
        shapes, scratch = [piece, piece], [block]
    else:
        operands += following[0:4]
        shapes, scratch = [block, second.shape], []
        if kind == "update":
            shapes = [block] + shapes
    return call(functools.partial(finish_kernel, kind), [core], operands, shapes, scratch)


def shards(view_a, view_b_own, spread_a, spread_b):
    planes, rows, count_x = view_a.shape
    cells = planes * rows
    short = 2 * (spread_a.shape[1] // 2 - planes // 2) * rows
    slabs = lax.axis_size("gz")
    per_slab = view_b_own.shape[0]
    first_y = view_a.reshape(cells, count_x)
    block, piece, ends = (cells, count_x), (cells // 2, count_x), (short, count_x)

    core = lax.axis_index("gy").astype(jnp.int32).reshape(1)
    swap = [(0, 1), (1, 0)]
    up = [[(2 * i + core, 2 * i + 2 + core) for i in range(slabs - 1)] for core in range(2)]
    down = [[(2 * i + 2 + core, 2 * i + core) for i in range(slabs - 1)] for core in range(2)]

    def table_of(step):
        return tables((spread_a, spread_b)[step // 2], step % 2 == 1, core, planes, rows, count_x)

    packed = pack(view_b_own, planes)
    lanes = packed.shape[1]
    arrived = lax.all_to_all(packed.reshape(slabs, -1, lanes), "gz", 0, 0, tiled=True)
    arrived = arrived.reshape(-1, lanes)
    keep, give = call(part_kernel, [core], [first_y], [piece, piece])
    got = lax.ppermute(give, "gy", swap)
    (first,) = call(join_kernel, [core], [keep, got], [block])
    table = table_of(0)
    order = ordering(count_x, per_slab)

    kept, kept_x, given = call(
        functools.partial(start_kernel, planes, per_slab), [core],
        [arrived, first_y, order, *table[0:2]], [piece, piece, block], [block, block],
    )
    got = lax.ppermute(given, "gy", swap)
    whole, ends_of = call(enter_kernel, [core], [kept_x, got, *table[2:4]], [block, ends], [block])

    for step in range(4):
        first_planes = lax.ppermute(whole, ("gz", "gy"), up[1] + down[0])
        side_planes = lax.ppermute(whole, "gy", swap)
        second_planes = lax.ppermute(ends_of, ("gz", "gy"), up[0] + down[1])
        if step < 3:
            following = table_of(step + 1)
        part = partial([(*table[4:6], whole), (*table[6:8], side_planes)])
        forward_planes = lax.ppermute(first_planes, "gy", swap)
        part = partial([(*table[8:10], first_planes)], [part])
        if step == 0:
            second, estimate = call(join_both_kernel, [core], [kept, got, first], [block, block])
        part = partial([(*table[10:12], forward_planes)], [part])
        arrivals = (core, part, second_planes, table)
        if step % 2 == 0:
            measured = first if step == 0 else second
            whole, ends_of = finish("quotient", *arrivals, measured, following)
        elif step < 3:
            estimate, whole, ends_of = finish("update", *arrivals, estimate, following)
        else:
            keep, give = finish("last", *arrivals, estimate, None)
        table = following
    got = lax.ppermute(give, "gy", swap)
    (estimate,) = call(join_kernel, [core], [keep, got], [block])
    return estimate.reshape(planes, rows, count_x)


def solution(mesh):
    in_specs = (P(("blocks", "gz"), "gy", None), P(("blocks", "gz"), "gy", None), P(), P())
    out_specs = P(("blocks", "gz"), "gy", None)
    return jax.shard_map(shards, mesh=mesh, in_specs=in_specs, out_specs=out_specs, check_vma=False)
```
